32 devices in a mesh: expert: 4 (over z), tensor: 8 (over y, x, core).
Axes of the slice: x: 2, y: 2, z: 4, core: 2. Of those that a mesh axis runs over, the one named last changes fastest.
Arguments:
- stashed: bfloat16 [384, 4096], P('expert', 'tensor'), may hold values from -6 to 6
- expert_ids: int32 [384, 2], P('expert'), may hold values from 0 to 3, all different within a row; in each aligned block of 96 rows (0 to 95, 96 to 191, ...) at most 64 rows name the same one
- combine_weight: float32 [384, 2], P('expert'), may hold values from 0.2 to 1
- w_gate: bfloat16 [4, 7168, 4096], P('expert', 'tensor'), may hold values from -0.09375 to 0.09375
- w_up: bfloat16 [4, 7168, 4096], P('expert', 'tensor'), may hold values from -0.09375 to 0.09375
- w_down: bfloat16 [4, 7168, 4096], P('expert', 'tensor'), may hold values from -0.09375 to 0.09375
Outputs:
- mixed_out: bfloat16 [384, 4096], P('expert', 'tensor')
The draws below stay inside these ranges and needn't reach their ends.
Inputs may be any that keep to these rules, and one draw needn't show every extreme that they name: `expert_ids`: each row names two different experts. Among the 96 rows of one group (aligned blocks) no expert is named more than 64 times, and in some group some expert is named exactly 64 times.
All inputs are finite; a program needn't handle non-finite values.
Results may differ from the reference program's by a relative error of at most 0.0049.
Values may be sent and summed in bfloat16 or wider, within the bound.
A program may use at most 64 MiB of HBM per device.

```python
import math
import jax
import jax.numpy as jnp
import numpy as np
from jax import lax

D = 4096
FF = 7168
TOK_E = 96
EXPERTS = 4
TOKENS = 384
CAP = 64


def spiked(values, stream_key, source, target, blocks, factor):
    def block_of(position):
        return (jnp.arange(values.shape[position]) // (values.shape[position] // blocks)).reshape((-1,) + (1,) * (values.ndim - 1 - position))

    one_side = jax.random.permutation(stream_key, blocks)[block_of(target)]
    far = (block_of(target) + blocks // 2) % blocks
    return jnp.where((block_of(source) == one_side) | (block_of(source) == far), factor * values, values)


def block_levels(key, extent, pieces, low, top_value):
    def one(axis_at, shards_of):
        draws = jax.random.uniform(jax.random.fold_in(jax.random.fold_in(key, 6), axis_at), (shards_of,), jnp.float32, low / len(pieces), top_value / len(pieces))
        return jnp.repeat(jnp.exp(draws), extent[axis_at] // shards_of).reshape((-1,) + (1,) * (len(extent) - axis_at - 1))

    level = one(*pieces[0])
    for cut in pieces[1:]:
        level = level * one(*cut)
    return level


def shared_out(key, own, number, rows, number_of, top, limit, skew):
    ranking = jax.random.permutation(key, number_of)
    crowded, common = load_shares(number_of, rows * top, limit, skew, True), load_shares(number_of, rows * top, limit, skew, False)
    places = jnp.arange(number_of)

    def named(tallies, turn):
        used = int((tallies > 0).sum())
        fixed = max(1, used // 4)
        shifted = fixed + (places - fixed + turn * (used - fixed)) % max(1, number_of - fixed)
        return jnp.zeros((number_of,), jnp.int32).at[ranking[jnp.where(places < fixed, places, shifted)]].set(jnp.asarray(tallies, jnp.int32))

    tallies = jnp.where(number % 4 == 0, named(crowded, number // 4), named(common, number - number // 4 - 1))
    mixed = jax.random.permutation(jax.random.fold_in(own, 3), number_of)
    donor, sink = mixed[0:number_of // 2 * 2:2], mixed[1:number_of // 2 * 2:2]
    room = jnp.minimum(tallies[donor] - 1, limit - tallies[sink]) // 2
    room = jnp.where((donor == ranking[0]) | (sink == ranking[0]) | (tallies[sink] == 0), 0, jnp.maximum(room, 0))
    shifted = jax.random.randint(jax.random.fold_in(own, 4), (number_of // 2,), 0, 1 << 20) % (room + 1)
    tallies = tallies.at[donor].add(-shifted).at[sink].add(shifted)
    items = jnp.searchsorted(jnp.cumsum(tallies), jnp.arange(rows * top), side="right").astype(jnp.int32)
    grid = items.reshape(top, rows).T
    grid = grid[jax.random.permutation(jax.random.fold_in(own, 1), rows)]
    turn = jax.random.randint(jax.random.fold_in(own, 2), (rows, 1), 0, top)
    return jnp.take_along_axis(grid, (jnp.arange(top)[None, :] + turn) % top, axis=1)


def load_shares(number_of, total, bound, lean, full):
    loads = [(1 << 20) // math.isqrt(standing ** lean) + 1 for standing in range(1, number_of + 1)]
    largest = bound if full else min(bound, max(-(-total // number_of), total * loads[0] // sum(loads)))
    least = 1 if total - largest >= number_of - 1 else 0
    counts, spare = [largest] + [least] * (number_of - 1), total - largest - least * (number_of - 1)
    while spare > 0:
        movable = [i for i in range(1, number_of) if counts[i] < largest] or [i for i in range(1, number_of) if counts[i] < bound]
        pool, left = sum([loads[i] for i in movable]), spare
        for i in movable:
            more = min(bound - counts[i], max(1, left * loads[i] // pool), spare)
            counts[i] = counts[i] + more
            spare = spare - more
    return np.array(counts)


def normal_values(key, extent, scale, bound, pieces=(), kind=jnp.bfloat16):
    entries = scale * jax.random.normal(key, extent, jnp.float32)
    if pieces:
        entries = entries * block_levels(key, extent, pieces, -0.22, 0.18)
    return jnp.clip(entries, -bound, bound).astype(kind)


def heavy_noise(stream_key, extent, scale, limit, cuts, heavy, kind=jnp.bfloat16):
    entries = scale * jax.random.normal(stream_key, extent, jnp.float32)
    if cuts:
        entries = entries * block_levels(stream_key, extent, cuts, -0.22, 0.18)
    return jnp.clip(spiked(entries, jax.random.fold_in(stream_key, 3), *heavy), -limit, limit).astype(kind)


def setup_inputs(seed: int = 0) -> dict:
    key_of = jax.random.split(jax.random.key(seed), 7)
    stashed = normal_values(key_of[0], (TOKENS, D), 1.0, 6.0, ((0, 4), (1, 8)))
    expert_ids_keys = jax.random.split(jax.random.fold_in(key_of[1], 1), TOKENS // TOK_E)
    expert_ids_turns = jax.random.permutation(jax.random.fold_in(key_of[1], 3), TOKENS // TOK_E)
    expert_ids = jax.vmap(lambda own, number: shared_out(jax.random.fold_in(key_of[1], 2), own, number, TOK_E, EXPERTS, 2, CAP, 2))(expert_ids_keys, expert_ids_turns).reshape((TOKENS, 2))
    combine_weight = jnp.clip(0.2 + 0.8 * jax.random.uniform(key_of[2], (TOKENS, 2), jnp.float32) ** block_levels(key_of[2], (TOKENS, 2), ((0, 4),), -0.2, 0.2), 0.2, 1.0)
    w_gate = normal_values(key_of[3], (EXPERTS, FF, D), D ** -0.5, 0.09375, ((0, 4), (1, 8)))
    w_up = normal_values(key_of[4], (EXPERTS, FF, D), D ** -0.5, 0.09375, ((0, 4), (1, 8)))
    w_down = heavy_noise(key_of[5], (EXPERTS, FF, D), FF ** -0.5, 0.09375, ((0, 4), (1, 8)), (1, 2, 8, 2.0))
    return dict(stashed=stashed, expert_ids=expert_ids, combine_weight=combine_weight, w_gate=w_gate, w_up=w_up, w_down=w_down)


def slot_targets(expert_ids, experts, capacity):
    flat_ids = expert_ids.reshape(-1)
    one_hot = (flat_ids[:, None] == jnp.arange(experts, dtype=jnp.int32)[None, :]).astype(jnp.int32)
    before = jnp.cumsum(one_hot, axis=0) - one_hot
    slot_index = jnp.sum(before * one_hot, axis=1)
    return (flat_ids * capacity + slot_index).astype(jnp.int32).reshape(expert_ids.shape)


def contract_last(left, right):
    return lax.dot_general(left, right, (((1,), (1,)), ((), ())), preferred_element_type=jnp.float32)


def reference(stashed, expert_ids, combine_weight, w_gate, w_up, w_down):
    groups = stashed.shape[0] // TOK_E
    width = stashed.shape[1]
    grouped_ids = expert_ids.reshape(groups, TOK_E, 2)
    targets = jax.vmap(lambda ids: slot_targets(ids, EXPERTS, CAP))(grouped_ids)
    grouped_tokens = stashed.reshape(groups, TOK_E, width)
    values = jnp.broadcast_to(grouped_tokens[:, :, None, :], (groups, TOK_E, 2, width))
    group_index = jnp.broadcast_to(jnp.arange(groups, dtype=jnp.int32)[:, None, None], targets.shape)
    buffer = jnp.zeros((groups, EXPERTS * CAP, width), jnp.bfloat16)
    buffer = buffer.at[group_index, targets].set(values)
    buffer = buffer.reshape(groups, EXPERTS, CAP, width).transpose(1, 0, 2, 3).reshape(EXPERTS, groups * CAP, width)

    def expert_layer(operands):
        rows_in, gate_w, up_w, down_w = operands
        gate_acts = contract_last(rows_in, gate_w)
        up_acts = contract_last(rows_in, up_w)
        hidden = (jax.nn.silu(gate_acts) * up_acts).astype(jnp.bfloat16)
        return jnp.dot(hidden, down_w, preferred_element_type=jnp.float32)

    expert_out = lax.map(expert_layer, (buffer, w_gate, w_up, w_down))
    expert_out = expert_out.reshape(EXPERTS, groups, CAP, width).transpose(1, 0, 2, 3).reshape(groups, EXPERTS * CAP, width)
    gathered_out = expert_out[group_index, targets]
    weights = combine_weight.reshape(groups, TOK_E, 2)
    mixed_out = jnp.sum(weights[:, :, :, None] * gathered_out, axis=2)
    return mixed_out.reshape(groups * TOK_E, width).astype(jnp.bfloat16)
```

```python
import functools
import math

import jax
import jax.numpy as jnp
from jax import lax
from jax.experimental import pallas as pl
from jax.experimental.pallas import tpu as pltpu
from jax.sharding import PartitionSpec as P


def slot_targets(expert_ids, experts, capacity):
    flat_ids = expert_ids.reshape(-1)
    one_hot = (flat_ids[:, None] == jnp.arange(experts, dtype=jnp.int32)[None, :]).astype(jnp.int32)
    before = jnp.cumsum(one_hot, axis=0) - one_hot
    slot_index = jnp.sum(before * one_hot, axis=1)
    return (flat_ids * capacity + slot_index).reshape(expert_ids.shape)


def contract_last(left, right):
    return lax.dot_general(
        left, right, (((1,), (1,)), ((), ())), preferred_element_type=jnp.float32
    )


def contract_first(left, right):
    return lax.dot_general(
        left, right, (((0,), (0,)), ((), ())), preferred_element_type=jnp.float32
    )


def shards(stashed, expert_ids, combine_weight, w_gate, w_up, w_down):
    tok_count = stashed.shape[0]
    feat_width = stashed.shape[1]
    experts = lax.axis_size("expert")
    capacity = min(tok_count, 8 * tok_count // (3 * experts))
    targets = slot_targets(expert_ids, experts, capacity)
    columns = jnp.arange(experts * capacity, dtype=jnp.int32)
    pair_match = (targets[:, :, None] == columns[None, None, :]).astype(jnp.float32)
    selector = jnp.sum(pair_match, axis=1).T.astype(jnp.bfloat16)
    mixing = jnp.sum(pair_match * combine_weight[:, :, None], axis=1)
    gate_w = w_gate[0]
    up_w = w_up[0]
    down_w = w_down[0]
    gathered = lax.all_gather(stashed, "tensor", axis=1, tiled=True)
    outgoing = jnp.dot(selector, gathered, preferred_element_type=jnp.float32).astype(jnp.bfloat16)
    outgoing = outgoing.reshape(experts, capacity, gathered.shape[1])
    received = lax.all_to_all(outgoing, "expert", split_axis=0, concat_axis=0, tiled=True)
    sources, item_count, full_width = received.shape
    rows_in = received.reshape(sources * item_count, full_width)
    gate_acts = contract_last(rows_in, gate_w)
    up_acts = contract_last(rows_in, up_w)
    hidden = (jax.nn.silu(gate_acts) * up_acts).astype(jnp.bfloat16)
    result = jnp.dot(hidden, down_w, preferred_element_type=jnp.float32)
    partial_value = result.reshape(sources, item_count, result.shape[1])
    partial_value = partial_value.reshape(-1, partial_value.shape[2])
    own_share = lax.psum_scatter(partial_value, "tensor", scatter_dimension=1, tiled=True)
    returned_rows = lax.all_to_all(
        own_share.reshape(experts, capacity, feat_width),
        "expert",
        split_axis=0,
        concat_axis=0,
        tiled=True,
    )
    combined = jnp.dot(
        mixing,
        returned_rows.reshape(experts * capacity, feat_width),
        precision=lax.Precision.HIGHEST,
        preferred_element_type=jnp.float32,
    )
    return combined.astype(jnp.bfloat16)


MESH = pl.DeviceIdType.MESH


def flip(index, bit):
    return index + bit - 2 * bit * lax.rem(lax.div(index, bit), 2)


def layer_kernel(
    groups, cap,
    x_hbm, ids_hbm, cw_hbm, wg_hbm, wu_hbm, wd_hbm, out_ref,
    x_ref, ids_ref, cw_ref, wg, wu, wd, picked, rows_in, gate_acc, up_acc, hidden,
    sib_out, sib_in, own_part, d_out, d_in, x_out, y_out, xy_in, z_out, z_in,
    in_sem, w_sem, send_sem, recv_sem,
):
    tokens, feat = x_ref.shape
    part = feat // 2
    z = lax.axis_index("expert")
    t = lax.axis_index("tensor")
    core = lax.rem(t, 2)
    sib, tx, ty = flip(t, 1), flip(t, 2), flip(t, 4)
    td = flip(tx, 4)
    chip_of = [lax.div(owner, 2) for owner in (t, tx, ty, td)]
    group_of = [z, flip(z, 1), flip(z, 2), flip(flip(z, 1), 2)]
    steps, halves = range(groups), range(2)

    barrier = pltpu.get_barrier_semaphore()
    peers = [{"expert": group_of[s]} for s in steps[1:]]
    peers += [{"tensor": tx}, {"tensor": ty}, {"tensor": td}, {"tensor": sib}]
    for peer in peers:
        pl.semaphore_signal(barrier, inc=1, device_id=peer, device_id_type=MESH)

    inputs = []
    for i, (hbm, vmem) in enumerate(((ids_hbm, ids_ref), (x_hbm, x_ref), (cw_hbm, cw_ref))):
        inputs.append(pltpu.make_async_copy(hbm, vmem, in_sem.at[i]))
    loads = []
    for i, (hbm, vmem) in enumerate(((wg_hbm, wg), (wu_hbm, wu), (wd_hbm, wd))):
        half = vmem.shape[0] // 2
        for j in halves:
            at = pl.ds(j * half, half)
            loads.append(pltpu.make_async_copy(hbm.at[0, at], vmem.at[at], w_sem.at[i]))
    for load in inputs:
        load.start()

    earlier = (
        lax.broadcasted_iota(jnp.int32, (tokens, tokens), 0)
        < lax.broadcasted_iota(jnp.int32, (tokens, tokens), 1)
    ).astype(jnp.bfloat16)
    experts_at = lax.broadcasted_iota(jnp.int32, (8, tokens), 0)
    slots = lax.broadcasted_iota(jnp.int32, (groups * cap, tokens), 0).astype(jnp.float32)
    inputs[0].wait()
    ids = ids_ref[...]
    first = (ids[0:1] == experts_at).astype(jnp.float32)
    second = (ids[1:2] == experts_at).astype(jnp.float32)
    before = jnp.dot((first + second).astype(jnp.bfloat16), earlier, preferred_element_type=jnp.float32)
    slot0 = jnp.sum(before * first, axis=0, keepdims=True)
    slot1 = jnp.sum((before + first) * second, axis=0, keepdims=True)
    place = (ids ^ z).astype(jnp.float32) * cap
    match0 = (slots == place[0:1] + slot0).astype(jnp.float32)
    match1 = (slots == place[1:2] + slot1).astype(jnp.float32)
    selector = (match0 + match1).astype(jnp.bfloat16)
    inputs[1].wait()
    for load in loads:
        load.start()
    chosen = jnp.dot(selector, x_ref[...], preferred_element_type=jnp.float32).astype(jnp.bfloat16)
    for h in halves:
        lanes = slice(h * part, (h + 1) * part)
        picked[h] = chosen[cap:, lanes]
        rows_in[0, h, 0, 0:cap] = chosen[:cap, lanes]

    numbers, sent = {}, []
    straight = ()
    straight_back = ()

    def remote(key, src, dst, peer):
        number = numbers.setdefault(key, len(numbers))
        return pltpu.make_async_remote_copy(
            src_ref=src, dst_ref=dst, send_sem=send_sem.at[0], recv_sem=recv_sem.at[number],
            device_id=peer, device_id_type=MESH,
        )

    def send(key, src, dst, peer):
        sent.append(math.prod(src.shape))
        remote(key, src, dst, peer).start()

    def arrive(key, dst):
        remote(key, dst, dst, {"tensor": sib}).wait_recv()

    def wait_load(hbm, vmem, i):
        pltpu.make_async_copy(hbm.at[0], vmem, w_sem.at[i]).wait()

    def rows_of(s):
        return pl.ds(s * cap, cap)

    def block(q, h, r, s):
        return rows_in.at[q, h, r, rows_of(s)]

    def send_z(s, h):
        send(("z", s, h), picked.at[h, rows_of(s - 1)], block(0, h, 0, s), {"expert": group_of[s]})

    def own(s, h):
        here = block(0, h, 0, s)
        if s > 0:
            arrive(("z", s, h), here)
        send(("x", s, h), here, block(1, h, 0, s), {"tensor": tx})
        send(("y", s, h), here, block(2, h, 0, s), {"tensor": ty})
        send(("s", 0, h), here, block(0, h, 1, s), {"tensor": sib})

    def far(s, h):
        send(("d", s, h), block(0, h, 0, s), block(3, h, 0, s), {"tensor": td})

    def pass_x(s, h):
        here = block(1, h, 0, s)
        arrive(("x", s, h), here)
        if (s + h) % 2 == 0 and (s, h) not in straight:
            send(("d", s, h), here, block(3, h, 0, s), {"tensor": ty})
        send(("s", 1, h), here, block(1, h, 1, s), {"tensor": sib})

    def pass_y(s, h):
        here = block(2, h, 0, s)
        arrive(("y", s, h), here)
        if (s + h) % 2 == 1 and (s, h) not in straight:
            send(("d", s, h), here, block(3, h, 0, s), {"tensor": tx})
        send(("s", 2, h), here, block(2, h, 1, s), {"tensor": sib})

    def pass_d(s, h):
        here = block(3, h, 0, s)
        arrive(("d", s, h), here)
        send(("s", 3, h), here, block(3, h, 1, s), {"tensor": sib})

    started = []

    def project(q, h):
        arrive(("s", q, h), rows_in.at[q, h, 1])
        for weight, acc in ((wg, gate_acc), (wu, up_acc)):
            value = None if not started else acc[...]
            for r in range(2):
                at = chip_of[q] * (2 * feat) + (core ^ r) * feat + h * part
                lanes = pl.ds(pl.multiple_of(at, part), part)
                term = contract_last(rows_in[q, h, r], weight[:, lanes])
                value = term if value is None else value + term
            acc[...] = value
        started.append(q)

    pl.semaphore_wait(barrier, len(peers))
    for s, h in ((1, 0), (1, 1), (2, 0), (3, 0), (2, 1), (3, 1)): send_z(s, h)
    own(0, 0)
    own(0, 1)
    pass_x(0, 0)
    pass_y(0, 0)
    own(1, 0)
    pass_x(0, 1)
    pass_y(0, 1)
    own(1, 1)
    own(2, 0)
    own(3, 0)
    pass_x(1, 0)
    pass_y(1, 0)
    pass_x(1, 1)
    pass_y(1, 1)
    pass_d(0, 0)
    pass_d(0, 1)
    wait_load(wg_hbm, wg, 0)
    wait_load(wu_hbm, wu, 1)
    project(0, 0)
    pass_x(2, 0)
    pass_y(2, 0)
    pass_x(3, 0)
    pass_y(3, 0)
    own(2, 1)
    own(3, 1)
    pass_d(1, 0)
    pass_d(1, 1)
    project(0, 1)
    project(1, 0)
    pass_x(2, 1)
    pass_y(2, 1)
    project(2, 0)
    pass_x(3, 1)
    pass_y(3, 1)
    pass_d(2, 0)
    pass_d(3, 0)
    project(3, 0)
    project(1, 1)
    pass_d(2, 1)
    pass_d(3, 1)
    project(2, 1)
    project(3, 1)

    wide = 2 * feat
    half_rows = groups * cap // 2

    def activate(j):
        at = pl.ds(j * half_rows, half_rows)
        gate = gate_acc[at]
        hidden[at] = (gate / (1.0 + jnp.exp(-gate)) * up_acc[at]).astype(jnp.bfloat16)

    def down(q, j):
        at = pl.ds(j * half_rows, half_rows)
        lanes = pl.ds(pl.multiple_of(chip_of[q] * wide, wide), wide)
        value = jnp.dot(hidden[at], wd[:, lanes], preferred_element_type=jnp.float32)
        low, high = value[:, :feat], value[:, feat:]
        sib_out[q, at] = jnp.where(core == 0, high, low).astype(jnp.bfloat16)
        send(("sum", q, j), sib_out.at[q, at], sib_in.at[q, at], {"tensor": sib})
        own_part[q, at] = jnp.where(core == 0, low, high)

    def chip_sum(q, s, h):
        if ("sum", q, s // 2) not in summed:
            at = pl.ds(s // 2 * half_rows, half_rows)
            arrive(("sum", q, s // 2), sib_in.at[q, at])
            summed.append(("sum", q, s // 2))
        rows, lanes = slice(s * cap, (s + 1) * cap), slice(h * part, (h + 1) * part)
        return own_part[q, rows, lanes] + sib_in[q, rows, lanes].astype(jnp.float32)

    summed = []

    def sum_d(s, h):
        d_out[s, h] = chip_sum(3, s, h).astype(jnp.bfloat16)
        peer = tx if (s + h) % 2 == 0 else ty
        send(("sd", s, h), d_out.at[s, h], d_in.at[s, h], {"tensor": td if (s, h) in straight_back else peer})

    def diagonal(s, h):
        arrive(("sd", s, h), d_in.at[s, h])
        return d_in[s, h].astype(jnp.float32)

    def sum_x(s, h):
        value = chip_sum(1, s, h)
        if (s + h) % 2 == 1 and (s, h) not in straight_back:
            value = value + diagonal(s, h)
        x_out[s, h] = value.astype(jnp.bfloat16)
        send(("sxy", s, h), x_out.at[s, h], xy_in.at[s, h, 0], {"tensor": tx})

    def sum_y(s, h):
        value = chip_sum(2, s, h)
        if (s + h) % 2 == 0 and (s, h) not in straight_back:
            value = value + diagonal(s, h)
        y_out[s, h] = value.astype(jnp.bfloat16)
        send(("sxy", s, h), y_out.at[s, h], xy_in.at[s, h, 1], {"tensor": ty})

    def total(s, h):
        value = chip_sum(0, s, h)
        if (s, h) in straight_back:
            value = value + diagonal(s, h)
        arrive(("sxy", s, h), xy_in.at[s, h])
        value = value + xy_in[s, h, 0].astype(jnp.float32) + xy_in[s, h, 1].astype(jnp.float32)
        if s == 0:
            z_in[h, rows_of(0)] = value.astype(jnp.bfloat16)
        else:
            z_out[s, h] = value.astype(jnp.bfloat16)
            send("back", z_out.at[s, h], z_in.at[h, rows_of(s)], {"expert": group_of[s]})

    activate(1)
    wait_load(wd_hbm, wd, 2)
    down(3, 1)
    down(1, 1)
    sum_d(2, 0)
    sum_d(2, 1)
    sum_d(3, 0)
    sum_d(3, 1)
    down(2, 1)
    sum_x(2, 0)
    sum_x(3, 1)
    down(0, 1)
    sum_y(2, 1)
    sum_y(3, 0)
    activate(0)
    down(3, 0)
    down(1, 0)
    sum_y(2, 0)
    sum_x(2, 1)
    sum_d(1, 0)
    sum_d(1, 1)
    sum_x(3, 0)
    sum_y(3, 1)
    down(2, 0)
    sum_x(1, 1)
    sum_y(1, 0)
    sum_d(0, 0)
    sum_d(0, 1)
    down(0, 0)
    total(2, 0)
    total(2, 1)
    sum_x(0, 0)
    sum_y(0, 1)
    total(3, 0)
    total(3, 1)
    sum_x(1, 0)
    sum_y(1, 1)
    sum_y(0, 0)
    sum_x(0, 1)
    total(1, 0)
    total(1, 1)
    total(0, 0)
    total(0, 1)

    inputs[2].wait()
    weights = cw_ref[...]
    mixing = match0 * weights[0:1] + match1 * weights[1:2]
    coarse = mixing.astype(jnp.bfloat16)
    fine = (mixing - coarse.astype(jnp.float32)).astype(jnp.bfloat16)
    returned = pl.ds(cap, (groups - 1) * cap)
    arrive("back", z_in.at[:, returned])
    for h in halves:
        combined = contract_first(coarse, z_in[h]) + contract_first(fine, z_in[h])
        out_ref[:, h * part:(h + 1) * part] = combined.astype(jnp.bfloat16)
    total_rows = sum(sent) // wg.shape[1]
    everything = wg.at[pl.ds(0, total_rows)]
    remote("back", everything, everything, {"tensor": sib}).wait_send()


def fused_shards(stashed, expert_ids, combine_weight, w_gate, w_up, w_down):
    groups = lax.axis_size("expert")
    tokens, feat = stashed.shape
    cap = min(tokens, 8 * tokens // (3 * groups))
    _, units, width = w_gate.shape
    rows = groups * cap
    part = feat // 2
    bf16, f32 = jnp.bfloat16, jnp.float32
    hbm = pl.BlockSpec(memory_space=pl.ANY)
    piece = pltpu.VMEM((groups, 2, cap, part), bf16)
    return pl.pallas_call(
        functools.partial(layer_kernel, groups, cap),
        out_shape=pltpu.VMEM((tokens, feat), bf16),
        in_specs=[hbm] * 6,
        out_specs=pl.BlockSpec(memory_space=pltpu.VMEM),
        scratch_shapes=[
            pltpu.VMEM((tokens, feat), bf16),
            pltpu.VMEM((2, tokens), jnp.int32),
            pltpu.VMEM((2, tokens), f32),
            pltpu.VMEM((units, width), bf16),
            pltpu.VMEM((units, width), bf16),
            pltpu.VMEM((units, width), bf16),
            pltpu.VMEM((2, rows - cap, part), bf16),
            pltpu.VMEM((4, 2, 2, rows, part), bf16),
            pltpu.VMEM((rows, units), f32),
            pltpu.VMEM((rows, units), f32),
            pltpu.VMEM((rows, units), bf16),
            pltpu.VMEM((4, rows, feat), bf16),
            pltpu.VMEM((4, rows, feat), bf16),
            pltpu.VMEM((4, rows, feat), f32),
            piece,
            piece,
            piece,
            piece,
            pltpu.VMEM((groups, 2, 2, cap, part), bf16),
            piece,
            pltpu.VMEM((2, rows, part), bf16),
            pltpu.SemaphoreType.DMA((3,)),
            pltpu.SemaphoreType.DMA((3,)),
            pltpu.SemaphoreType.DMA((1,)),
            pltpu.SemaphoreType.DMA((63,)),
        ],
        compiler_params=pltpu.CompilerParams(
            collective_id=0, has_side_effects=True, vmem_limit_bytes=60 * 1024 * 1024
        ),
    )(stashed, expert_ids.T, combine_weight.T, w_gate, w_up, w_down)


def picks_kernel(mesh):
    return mesh.shape["tensor"] == 8 and mesh.shape["expert"] == 4


def solution(mesh):
    return jax.shard_map(
        fused_shards if picks_kernel(mesh) else shards,
        mesh=mesh,
        in_specs=(
            P("expert", "tensor"),
            P("expert", None),
            P("expert", None),
            P("expert", "tensor", None),
            P("expert", "tensor", None),
            P("expert", "tensor", None),
        ),
        out_specs=P("expert", "tensor"),
        check_vma=False,
    )
```
